32 devices in a mesh: depth: 4 (over z), sample: 4 (over y, x), filter: 2 (over core).
Axes of the slice: x: 2, y: 2, z: 4, core: 2. Of those that a mesh axis runs over, the one named last changes fastest.
Arguments:
- inputs: float32 [4, 8, 8, 8, 256], P('sample', 'depth', None, None, 'filter'), may hold values from -6 to 6
- pre_gelu: float32 [4, 8, 8, 8, 256], P('sample', 'depth', None, None, 'filter'), may hold values from -6 to 6
- output_grad: float32 [4, 8, 8, 8, 256], P('sample', 'depth', None, None, 'filter'), may hold values from -6 to 6
- first_weight: float32 [27, 256, 256], P(None, None, 'filter'), may hold values from -0.078125 to 0.078125
- second_weight: float32 [27, 256, 256], P(None, None, 'filter'), may hold values from -0.078125 to 0.078125
Outputs:
- input_grad: float32 [4, 8, 8, 8, 256], P('sample', 'depth', None, None, 'filter')
- first_weight_grad: float32 [27, 256, 256], P(None, 'depth', 'filter')
- second_weight_grad: float32 [27, 256, 256], P(None, 'depth', 'filter')
The draws below stay inside these ranges and needn't reach their ends.
All inputs are finite; a program needn't handle non-finite values.
Results may differ from the reference program's by a relative error of at most 0.000098.
Values sent between devices are 32-bit elements; how exact they have to be, the bound alone decides.
No kernel may reach another device: no remote copies, remote signals or barrier semaphores. Data moves between devices by JAX's collectives and lax.ppermute only.
A program may use at most 64 MiB of HBM per device.

```python
import math
import jax
import jax.numpy as jnp
from jax import lax

C = 256
GRID_H = 8
GRID_W = 8
SAMPLES = 4
NDEPTH = 8


def with_spikes(result, own_key, source, target, shards_of, factor):
    owner, partner = [(jnp.arange(result.shape[position]) // (result.shape[position] // shards_of)).reshape([-1 if axis == position else 1 for axis in range(result.ndim)]) for position in (source, target)]
    chosen = jax.random.permutation(own_key, shards_of)[partner]
    strong = (owner == chosen) | (owner == (partner + shards_of // 2) % shards_of)
    return jnp.where(strong, factor * result, result)


def steps_of(stream_key, extent, shards, low, high):
    loudness = 1.0
    for position, parts in shards:
        steps = jax.random.uniform(jax.random.fold_in(jax.random.fold_in(stream_key, 6), position), (parts,), jnp.float32, low / len(shards), high / len(shards))
        loudness = loudness * jnp.repeat(jnp.exp(steps), extent[position] // parts).reshape((-1,) + (1,) * (len(extent) - 1 - position))
    return loudness


def scatter_about(rng, extent, deviation, bound, shards=(), kind=jnp.bfloat16):
    result = jax.random.normal(rng, extent, jnp.float32) * deviation
    if len(shards) > 0:
        result = steps_of(rng, extent, shards, -0.22, 0.18) * result
    return jnp.clip(result, min=-bound, max=bound).astype(kind)


def noise_with(stream_key, dims, deviation, bound, pieces, heavy, kind=jnp.bfloat16):
    result = deviation * jax.random.normal(stream_key, dims, jnp.float32)
    if pieces:
        result = result * steps_of(stream_key, dims, pieces, -0.22, 0.18)
    return jnp.clip(with_spikes(result, jax.random.fold_in(stream_key, 3), *heavy), -bound, bound).astype(kind)


def setup_inputs(seed: int = 0) -> dict:
    seeds = jax.random.split(jax.random.key(seed), 6)
    return {
        "inputs": noise_with(seeds[0], (SAMPLES, NDEPTH, GRID_H, GRID_W, C), 1.0, 6.0, ((0, 4), (1, 4), (4, 2)), (1, 4, 4, 2.0), jnp.float32),
        "pre_gelu": noise_with(seeds[1], (SAMPLES, NDEPTH, GRID_H, GRID_W, C), 1.0, 6.0, ((0, 4), (1, 4), (4, 2)), (1, 4, 4, 2.0), jnp.float32),
        "output_grad": scatter_about(seeds[2], (SAMPLES, NDEPTH, GRID_H, GRID_W, C), 1.0, 6.0, ((0, 4), (1, 4), (4, 2)), jnp.float32),
        "first_weight": scatter_about(seeds[3], (27, C, C), (27 * C) ** -0.5, 0.078125, ((2, 2),), jnp.float32),
        "second_weight": scatter_about(seeds[4], (27, C, C), (27 * C) ** -0.5, 0.078125, ((2, 2),), jnp.float32),
    }


def gelu_pair(pre):
    normal_cdf = 0.5 * (1.0 + lax.erf(pre * 0.7071067811865476))
    density = jnp.exp(-0.5 * pre * pre) * 0.3989422804014327
    return (pre * normal_cdf, normal_cdf + pre * density)

def conv_same(field, kernel_flat):
    kernel = kernel_flat.reshape(3, 3, 3, kernel_flat.shape[1], kernel_flat.shape[2])
    return lax.conv_general_dilated(field, kernel, (1, 1, 1), ((1, 1), (1, 1), (1, 1)), dimension_numbers=('NDHWC', 'DHWIO', 'NDHWC'), precision=lax.Precision.HIGHEST)

def reference(inputs, pre_gelu, output_grad, first_weight, second_weight):
    activated, slope = gelu_pair(pre_gelu)
    unused_second, second_back = jax.vjp(conv_same, activated, second_weight)
    act_grad, second_raw = second_back(output_grad)
    pre_grad = act_grad * slope
    unused_first, first_back = jax.vjp(conv_same, inputs, first_weight)
    input_grad, first_raw = first_back(pre_grad)
    cells = inputs.shape[0] * inputs.shape[1] * inputs.shape[2] * inputs.shape[3]
    factor = 1.0 / math.sqrt(cells)
    return (input_grad, first_raw * factor, second_raw * factor)
```

```python
import functools
import math

import jax
import jax.numpy as jnp
from jax import lax
from jax.experimental import pallas as pl
from jax.experimental.pallas import tpu as pltpu
from jax.sharding import PartitionSpec as P

highest = lax.Precision.HIGHEST


def padded_2(cells, sides, width):
    for axis, dim in sides:
        count = lax.axis_size(axis)
        ends = count - 1
        head = lax.slice_in_dim(cells, 0, width, axis=dim)
        tail = lax.slice_in_dim(cells, cells.shape[dim] - width, cells.shape[dim], axis=dim)
        cells = jnp.concatenate(
            [
                lax.ppermute(tail, axis, [(i, (i + 1) % count) for i in range(ends)]),
                cells,
                lax.ppermute(head, axis, [((i + 1) % count, i) for i in range(ends)]),
            ],
            axis=dim,
        )
    return cells


def gelu_pair(pre):
    normal_cdf = 0.5 * (1.0 + lax.erf(pre * 0.7071067811865476))
    density = jnp.exp(-0.5 * pre * pre) * 0.3989422804014327
    return (pre * normal_cdf, normal_cdf + pre * density)


def pad_sides(field):
    return jnp.pad(field, [(0, 0)] * (field.ndim - 3) + [(1, 1), (1, 1), (0, 0)])


def patches(padded, flipped):
    planes = padded.shape[-4] - 2
    height = padded.shape[-3] - 2
    breadth = padded.shape[-2] - 2
    pieces = []
    for depth_tap in range(3):
        for row_tap in range(3):
            for column_tap in range(3):
                start_plane = 2 - depth_tap if flipped else depth_tap
                start_row = 2 - row_tap if flipped else row_tap
                start_column = 2 - column_tap if flipped else column_tap
                pieces.append(
                    padded[
                        ...,
                        start_plane : start_plane + planes,
                        start_row : start_row + height,
                        start_column : start_column + breadth,
                        :,
                    ]
                )
    stacked = jnp.stack(pieces, axis=-2)
    return stacked.reshape(-1, 27, padded.shape[-1])


def spread_back(grad_local, kernel):
    planes = padded_2(grad_local, (("depth", 1),), 1)
    columns = patches(pad_sides(planes), True)
    partial_value = jnp.einsum("rtc,tic->ri", columns, kernel, precision=highest)
    partial_value = partial_value.reshape(grad_local.shape[:4] + (kernel.shape[1],))
    return lax.psum_scatter(partial_value, "filter", scatter_dimension=4, tiled=True)


def reduce_weight(raw_pair):
    summed = lax.psum(raw_pair, "sample")
    return lax.psum_scatter(summed, "depth", scatter_dimension=1, tiled=True)


def axis_sizes():
    return lax.axis_size("depth"), lax.axis_size("sample"), lax.axis_size("filter")


def gather_plan_fits(inputs, output_grad, second_weight):
    depths, samples, halves = axis_sizes()
    batch, planes, height, breadth, lanes = output_grad.shape
    rows = batch * samples * planes * depths * height * breadth
    return (
        batch == 1
        and halves == 2
        and lanes == 128
        and breadth == 8
        and height % 2 == 0
        and second_weight.shape[1] == halves * lanes
        and 2 * second_weight.shape[1] == depths * lanes
        and samples & (samples - 1) == 0
        and rows * lanes * 4 <= 2**21
    )


def column_shift(cells, tap):
    if tap == 1:
        return cells
    breadth = cells.shape[1]
    rolled = pltpu.roll(cells, 1 if tap == 0 else breadth - 1, axis=1)
    column = lax.broadcasted_iota(jnp.int32, cells.shape, 1)
    return jnp.where(column == (0 if tap == 0 else breadth - 1), 0.0, rolled)


def two_parts(cells):
    high = cells.astype(jnp.bfloat16)
    return high, (cells - high.astype(jnp.float32)).astype(jnp.bfloat16)


def row_pairs(cells):
    height, breadth, lanes = cells.shape
    edge = jnp.zeros((1, breadth, lanes), jnp.float32)
    even = jnp.concatenate([edge, cells, edge], axis=0)
    even = even.reshape(height // 2 + 1, 2 * breadth, lanes)
    return even, cells.reshape(height // 2, 2 * breadth, lanes)


def spread_field(get_plane, planes, even_ref, odd_ref):
    for plane in range(planes):
        source = get_plane(plane)
        for tap in range(3):
            even, odd = row_pairs(column_shift(source, tap))
            for part, value in enumerate(two_parts(even)):
                even_ref[tap, part, plane] = value
            for part, value in enumerate(two_parts(odd)):
                odd_ref[tap, part, plane] = value


def slab(even_ref, odd_ref, lead, first, planes, row_tap):
    pairs = odd_ref.shape[-3]
    where = pl.ds(first, planes)
    if row_tap == 1:
        value = odd_ref[(*lead, where)]
    else:
        start = row_tap // 2
        value = even_ref[(*lead, where, slice(start, start + pairs))]
    return value.reshape(-1, value.shape[-1])


def back_step(first, planes, weight_ref, even_ref, odd_ref, cells_first):
    height = weight_ref.shape[1]
    total = None
    for row_tap in range(3):
        left = []
        right = []
        for column_tap in range(3):
            kernel_high, kernel_low = two_parts(weight_ref[3 * row_tap + column_tap])
            cell = [
                slab(even_ref, odd_ref, (2 - column_tap, part), first, planes, 2 - row_tap)
                for part in range(2)
            ]
            left += [cell[0], cell[1], cell[0]]
            right += [kernel_high, kernel_high, kernel_low]
        left = jnp.concatenate(left, axis=1)
        right = jnp.concatenate(right, axis=1)
        if not cells_first:
            left, right = right, left
        product = lax.dot_general(
            left, right, (((1,), (1,)), ((), ())), preferred_element_type=jnp.float32
        )
        total = product if total is None else total + product
    return total


def split_halves(total, keep_ref, send_ref):
    width = keep_ref.shape[-1]
    mine = lax.axis_index("filter") == 0
    low, high = total[:, :width], total[:, width:]
    keep_ref[...] = jnp.where(mine, low, high)
    send_ref[...] = jnp.where(mine, high, low)


def act_back_kernel(field_ref, weight_ref, keep_ref, send_ref, even_ref, odd_ref, total_ref):
    step = pl.program_id(0)
    planes = field_ref.shape[0]

    @pl.when(step == 0)
    def _():
        for ref in (even_ref, odd_ref):
            for tap in range(3):
                for part in range(2):
                    for plane in (0, planes + 1):
                        ref[tap, part, plane] = jnp.zeros(ref.shape[3:], ref.dtype)
        spread_field(
            lambda plane: field_ref[plane],
            planes,
            even_ref.at[:, :, 1 : planes + 1],
            odd_ref.at[:, :, 1 : planes + 1],
        )
        total_ref[...] = jnp.zeros_like(total_ref)

    total_ref[...] += back_step(2 - step, planes, weight_ref, even_ref, odd_ref, True)

    @pl.when(step == 2)
    def _():
        split_halves(total_ref[...], keep_ref, send_ref)


def input_back_kernel(planes, field_ref, weight_ref, keep_ref, send_ref, even_ref, odd_ref, total_ref):
    step = pl.program_id(0)
    depths = field_ref.shape[0]

    @pl.when(step == 0)
    def _():
        first = lax.axis_index("depth") * planes

        def plane_at(offset):
            place = first + offset - 1
            inside = (place >= 0) & (place < depths)
            return jnp.where(inside, field_ref[jnp.clip(place, 0, depths - 1)], 0.0)

        spread_field(plane_at, planes + 2, even_ref, odd_ref)
        total_ref[...] = jnp.zeros_like(total_ref)

    total_ref[...] += back_step(2 - step, planes, weight_ref, even_ref, odd_ref, False)

    @pl.when(step == 2)
    def _():
        split_halves(total_ref[...].T, keep_ref, send_ref)


def full_spec(shape):
    return pl.BlockSpec(shape, lambda *_: (0,) * len(shape))


def spread_scratch(planes, height, breadth, lanes, parts):
    return [
        pltpu.VMEM((3, parts, planes, height // 2 + 1, 2 * breadth, lanes), jnp.bfloat16),
        pltpu.VMEM((3, parts, planes, height // 2, 2 * breadth, lanes), jnp.bfloat16),
    ]


def spread_call(field, kernel, planes, whole):
    depths, height, breadth, lanes = field.shape
    taps, ins, outs = kernel.shape
    rows = planes * height * breadth
    body = act_back_kernel if whole else functools.partial(input_back_kernel, planes)
    return pl.pallas_call(
        body,
        grid=(3,),
        in_specs=[
            full_spec(field.shape),
            pl.BlockSpec((taps // 3, ins, outs), lambda step: (step, 0, 0)),
        ],
        out_specs=[full_spec((rows, ins // 2))] * 2,
        out_shape=[jax.ShapeDtypeStruct((rows, ins // 2), jnp.float32)] * 2,
        scratch_shapes=spread_scratch(planes + 2, height, breadth, lanes, 2)
        + [pltpu.VMEM((rows, ins) if whole else (ins, rows), jnp.float32)],
        compiler_params=pltpu.CompilerParams(vmem_limit_bytes=48 * 2**20),
        cost_estimate=pl.CostEstimate(
            flops=6 * rows * taps * ins * outs, transcendentals=0, bytes_accessed=4 * kernel.size
        ),
        name="act_back" if whole else "input_back",
    )(field, kernel)


def join_kernel(*refs):
    *pieces, out_ref = refs
    count = len(pieces)
    planes = pieces[0].shape[0]
    place = lax.axis_index("depth")
    for step, piece in enumerate(pieces):
        source = lax.rem(place + count - step, count)
        out_ref[pl.ds(source * planes, planes)] = piece[...]


def join_depth(pieces):
    planes, *rest = pieces[0].shape
    return pl.pallas_call(
        join_kernel,
        out_shape=jax.ShapeDtypeStruct((planes * len(pieces), *rest), jnp.float32),
        name="join_depth",
    )(*pieces)


def activation_kernel(count, *refs):
    saved, before = refs[:count], refs[count : 2 * count]
    slope_ref, pair_ref = refs[2 * count :]
    planes = saved[0].shape[0]
    place = lax.axis_index("depth")
    lower = lax.rem(place, 2) == 0
    half = saved[0].shape[-1] // 2
    for step in range(count):
        source = lax.rem(place + count - step, count)
        where = pl.ds(source * planes, planes)
        shape = saved[step].shape
        first = saved[step][...].reshape(-1, shape[-1])
        activated, slope = gelu_pair(before[step][...].reshape(-1, shape[-1]))
        slope_ref[where] = slope.reshape(shape)
        lane = lax.broadcasted_iota(jnp.int32, first.shape, 1)
        low = jnp.where(lane < half, first, pltpu.roll(activated, half, axis=1))
        high = jnp.where(lane < half, pltpu.roll(first, half, axis=1), activated)
        pair_ref[where] = jnp.where(lower, low, high).reshape(shape)


def activation_call(saved, before):
    planes, *rest = saved[0].shape
    count = len(saved)
    shape = (planes * count, *rest)
    return pl.pallas_call(
        functools.partial(activation_kernel, count),
        out_shape=[jax.ShapeDtypeStruct(shape, jnp.float32)] * 2,
        name="activation",
    )(*saved, *before)


def weight_kernel(count, second, factor, *refs):
    fields, near, far = refs[:count], refs[count : 2 * count], refs[2 * count : 3 * count]
    out_ref, even_ref, odd_ref, grad_ref = refs[3 * count :]
    step = pl.program_id(0)
    planes, height, breadth, lanes = near[0].shape
    half = lanes // 2
    rows = planes * height * breadth

    @pl.when(step == 0)
    def _():
        owner = lax.axis_index("depth") // 2 == lax.axis_index("filter")
        for sample in range(count):
            for ref in (even_ref, odd_ref):
                for tap in range(3):
                    for plane in (0, planes + 1):
                        ref[tap, sample, plane] = jnp.zeros(ref.shape[3:], ref.dtype)
            for plane in range(planes):
                cells = jnp.where(owner, near[sample][plane], far[sample][plane])
                lane = lax.broadcasted_iota(jnp.int32, cells.shape, 2)
                swapped = pltpu.roll(cells, half, axis=2)
                lower = lane < half
                cells = jnp.where(lower, swapped, cells) if second else jnp.where(lower, cells, swapped)
                high = cells.astype(jnp.bfloat16).astype(jnp.float32)
                cells = jnp.where(lower, high, cells - high)
                for tap in range(3):
                    even, odd = row_pairs(column_shift(cells, tap))
                    even_ref[tap, sample, plane + 1] = even.astype(jnp.bfloat16)
                    odd_ref[tap, sample, plane + 1] = odd.astype(jnp.bfloat16)
            turned = fields[sample][...].reshape(rows, lanes).T
            for part, value in enumerate(two_parts(turned)):
                grad_ref[part * lanes : (part + 1) * lanes, sample * rows : (sample + 1) * rows] = value

    def cell(row_tap, column_tap):
        return jnp.concatenate(
            [
                slab(even_ref, odd_ref, (column_tap, sample), step, planes, row_tap)
                for sample in range(count)
            ],
            axis=0,
        )

    taps = [(row_tap, column_tap) for row_tap in range(3) for column_tap in range(3)]
    for start in range(0, 9, 2):
        group = taps[start : start + 2]
        right = [cell(*tap) for tap in group]
        right = jnp.concatenate(right, axis=1) if len(right) > 1 else right[0]
        product = jnp.dot(grad_ref[...], right, preferred_element_type=jnp.float32)
        product = product[:lanes] + product[lanes:]
        for index in range(len(group)):
            piece = product[:, index * lanes : (index + 1) * lanes]
            piece = piece + pltpu.roll(piece, half, axis=1)
            out_ref[start + index] = piece.T[:half] * factor


def weight_call(fields, near, far, second, factor):
    planes, height, breadth, lanes = near[0].shape
    count = len(fields)
    rows = planes * height * breadth
    scratch = [
        pltpu.VMEM((3, count, planes + 2, height // 2 + 1, 2 * breadth, lanes), jnp.bfloat16),
        pltpu.VMEM((3, count, planes + 2, height // 2, 2 * breadth, lanes), jnp.bfloat16),
        pltpu.VMEM((2 * lanes, count * rows), jnp.bfloat16),
    ]
    return pl.pallas_call(
        functools.partial(weight_kernel, count, second, factor),
        grid=(3,),
        in_specs=[full_spec(near[0].shape)] * (3 * count),
        out_specs=pl.BlockSpec((9, lanes // 2, lanes), lambda step: (step, 0, 0)),
        out_shape=jax.ShapeDtypeStruct((27, lanes // 2, lanes), jnp.float32),
        scratch_shapes=scratch,
        compiler_params=pltpu.CompilerParams(vmem_limit_bytes=56 * 2**20),
        cost_estimate=pl.CostEstimate(
            flops=4 * 2 * 27 * count * rows * lanes * lanes // 2,
            transcendentals=0,
            bytes_accessed=4 * 4 * count * rows * lanes,
        ),
        name="second_weight" if second else "first_weight",
    )(*fields, *near, *far)


def around_depth(field):
    count = lax.axis_size("depth")
    steps = [1, count - 1] + list(range(2, count - 1))
    moved = {
        step: lax.ppermute(field, "depth", [(i, (i + step) % count) for i in range(count)])
        for step in steps
    }
    return [field] + [moved[step] for step in range(1, count)]


def across_samples(field):
    count = lax.axis_size("sample")
    return [field] + [
        lax.ppermute(field, "sample", [(i, i ^ step) for i in range(count)])
        for step in range(1, count)
    ]


def owners_across_samples(pair):
    depths, samples, halves = axis_sizes()
    moved = [pair]
    for step in range(1, samples):
        links = []
        for depth in range(depths):
            for sample in range(samples):
                half = depth // 2
                place = lambda value: (depth * samples + value) * halves + half
                links.append((place(sample), place(sample ^ step)))
        moved.append(lax.ppermute(pair, ("depth", "sample", "filter"), links))
    return moved


def swap_filter(field):
    return lax.ppermute(field, "filter", [(0, 1), (1, 0)])


def gather_plan(inputs, pre_gelu, output_grad, first_weight, second_weight, factor):
    local_shape = output_grad.shape
    planes = local_shape[1]
    inputs, pre_gelu, output_grad = inputs[0], pre_gelu[0], output_grad[0]
    grads = join_depth(around_depth(output_grad))
    slope, pair = activation_call(around_depth(inputs), around_depth(pre_gelu))
    keep, send = spread_call(grads, second_weight, grads.shape[0], True)
    pre_grad = (keep + swap_filter(send)).reshape(slope.shape) * slope
    all_grads = across_samples(grads)
    near = owners_across_samples(pair)
    far = [swap_filter(piece) for piece in near]
    all_pre = across_samples(pre_grad)
    keep, send = spread_call(pre_grad, first_weight, planes, False)
    input_grad = (keep + swap_filter(send)).reshape(local_shape)
    second = weight_call(all_grads, near, far, True, factor)
    first = weight_call(all_pre, near, far, False, factor)
    return input_grad, first, second


def local(inputs, pre_gelu, output_grad, first_weight, second_weight):
    cells = (
        inputs.shape[0]
        * lax.axis_size("sample")
        * inputs.shape[1]
        * lax.axis_size("depth")
        * inputs.shape[2]
        * inputs.shape[3]
    )
    factor = 1.0 / math.sqrt(cells)
    if gather_plan_fits(inputs, output_grad, second_weight):
        return gather_plan(inputs, pre_gelu, output_grad, first_weight, second_weight, factor)
    activated, slope = gelu_pair(pre_gelu)
    stacked = jnp.stack([inputs, activated], axis=0)
    planes = padded_2(stacked, (("depth", 2),), 1)
    whole = lax.all_gather(planes, "filter", axis=5, tiled=True)
    padded = pad_sides(whole)
    local_width = output_grad.shape[4]
    act_columns = patches(padded[1], False)
    second_raw = jnp.einsum(
        "rti,rc->tic", act_columns, output_grad.reshape(-1, local_width), precision=highest
    )
    act_grad = spread_back(output_grad, second_weight)
    pre_grad = act_grad * slope
    input_grad = spread_back(pre_grad, first_weight)
    input_columns = patches(padded[0], False)
    first_raw = jnp.einsum(
        "rti,rc->tic", input_columns, pre_grad.reshape(-1, local_width), precision=highest
    )
    first_sum, second_sum = reduce_weight((first_raw, second_raw))
    return (input_grad, first_sum * factor, second_sum * factor)


def solution(mesh):
    return jax.shard_map(
        local,
        mesh=mesh,
        in_specs=(
            P("sample", "depth", None, None, "filter"),
            P("sample", "depth", None, None, "filter"),
            P("sample", "depth", None, None, "filter"),
            P(None, None, "filter"),
            P(None, None, "filter"),
        ),
        out_specs=(
            P("sample", "depth", None, None, "filter"),
            P(None, "depth", "filter"),
            P(None, "depth", "filter"),
        ),
        check_vma=False,
    )
```

```python
import functools
import itertools
import math

import jax
import jax.numpy as jnp
from jax import lax
from jax.experimental import pallas as pl
from jax.experimental.pallas import tpu as pltpu
from jax.sharding import PartitionSpec as P


highest = lax.Precision.HIGHEST


def padded_2(cells, sides, width):
    for axis, dim in sides:
        count = lax.axis_size(axis)
        ends = count - 1
        head = lax.slice_in_dim(cells, 0, width, axis=dim)
        tail = lax.slice_in_dim(cells, cells.shape[dim] - width, cells.shape[dim], axis=dim)
        cells = jnp.concatenate(
            [
                lax.ppermute(tail, axis, [(i, (i + 1) % count) for i in range(ends)]),
                cells,
                lax.ppermute(head, axis, [((i + 1) % count, i) for i in range(ends)]),
            ],
            axis=dim,
        )
    return cells


def gelu_pair(pre):
    normal_cdf = 0.5 * (1.0 + lax.erf(pre * 0.7071067811865476))
    density = jnp.exp(-0.5 * pre * pre) * 0.3989422804014327
    return (pre * normal_cdf, normal_cdf + pre * density)


def pad_sides(field):
    return jnp.pad(field, [(0, 0)] * (field.ndim - 3) + [(1, 1), (1, 1), (0, 0)])


def patches(padded, flipped):
    planes = padded.shape[-4] - 2
    height = padded.shape[-3] - 2
    breadth = padded.shape[-2] - 2
    pieces = []
    for depth_tap in range(3):
        for row_tap in range(3):
            for column_tap in range(3):
                start_plane = 2 - depth_tap if flipped else depth_tap
                start_row = 2 - row_tap if flipped else row_tap
                start_column = 2 - column_tap if flipped else column_tap
                pieces.append(
                    padded[
                        ...,
                        start_plane : start_plane + planes,
                        start_row : start_row + height,
                        start_column : start_column + breadth,
                        :,
                    ]
                )
    stacked = jnp.stack(pieces, axis=-2)
    return stacked.reshape(-1, 27, padded.shape[-1])


def spread_back(grad_local, kernel):
    planes = padded_2(grad_local, (("depth", 1),), 1)
    columns = patches(pad_sides(planes), True)
    partial_value = jnp.einsum("rtc,tic->ri", columns, kernel, precision=highest)
    partial_value = partial_value.reshape(grad_local.shape[:4] + (kernel.shape[1],))
    return lax.psum_scatter(partial_value, "filter", scatter_dimension=4, tiled=True)


def reduce_weight(raw_pair):
    summed = lax.psum(raw_pair, "sample")
    return lax.psum_scatter(summed, "depth", scatter_dimension=1, tiled=True)


def axis_sizes():
    return lax.axis_size("depth"), lax.axis_size("sample"), lax.axis_size("filter")


def gather_plan_fits(output_grad, second_weight):
    depths, samples, halves = axis_sizes()
    batch, planes, height, breadth, lanes = output_grad.shape
    rows = batch * samples * planes * depths * height * breadth
    return (
        batch == 1
        and halves == 2
        and lanes == 128
        and breadth == 8
        and height % 2 == 0
        and second_weight.shape[1] == halves * lanes
        and 2 * second_weight.shape[1] == depths * lanes
        and samples & (samples - 1) == 0
        and rows * lanes * 4 <= 2**21
    )


def column_shift(cells, tap):
    if tap == 1:
        return cells
    breadth = cells.shape[1]
    rolled = pltpu.roll(cells, 1 if tap == 0 else breadth - 1, axis=1)
    column = lax.broadcasted_iota(jnp.int32, cells.shape, 1)
    return jnp.where(column == (0 if tap == 0 else breadth - 1), 0.0, rolled)


def two_parts(cells):
    high = cells.astype(jnp.bfloat16)
    return high, (cells - high.astype(jnp.float32)).astype(jnp.bfloat16)


def row_pairs(cells):
    height, breadth, lanes = cells.shape
    edge = jnp.zeros((1, breadth, lanes), jnp.float32)
    even = jnp.concatenate([edge, cells, edge], axis=0)
    even = even.reshape(height // 2 + 1, 2 * breadth, lanes)
    return even, cells.reshape(height // 2, 2 * breadth, lanes)


def spread_field(get_plane, planes, even_ref, odd_ref):
    for plane in range(planes):
        source = get_plane(plane)
        for tap in range(3):
            even, odd = row_pairs(column_shift(source, tap))
            for part, value in enumerate(two_parts(even)):
                even_ref[tap, part, plane] = value
            for part, value in enumerate(two_parts(odd)):
                odd_ref[tap, part, plane] = value


def slab(even_ref, odd_ref, lead, first, planes, row_tap):
    pairs = odd_ref.shape[-3]
    where = pl.ds(first, planes)
    if row_tap == 1:
        value = odd_ref[(*lead, where)]
    else:
        start = row_tap // 2
        value = even_ref[(*lead, where, slice(start, start + pairs))]
    return value.reshape(-1, value.shape[-1])


def back_step(first, planes, weight_ref, even_ref, odd_ref):
    total = None
    for row_tap in range(3):
        cells = []
        kernels = []
        for column_tap in range(3):
            kernel_high, kernel_low = two_parts(weight_ref[3 * row_tap + column_tap])
            cell = [
                slab(even_ref, odd_ref, (2 - column_tap, part), first, planes, 2 - row_tap)
                for part in range(2)
            ]
            cells += [cell[0], cell[1], cell[0]]
            kernels += [kernel_high, kernel_high, kernel_low]
        product = lax.dot_general(
            jnp.concatenate(kernels, axis=1),
            jnp.concatenate(cells, axis=1),
            (((1,), (1,)), ((), ())),
            preferred_element_type=jnp.float32,
        )
        total = product if total is None else total + product
    return total


def split_halves(total, keep_ref, send_ref):
    width = keep_ref.shape[-1]
    mine = lax.axis_index("filter") == 0
    low, high = total[:, :width], total[:, width:]
    keep_ref[...] = jnp.where(mine, low, high).reshape(keep_ref.shape)
    send_ref[...] = jnp.where(mine, high, low).reshape(send_ref.shape)


def back_kernel(before_ref, own_ref, after_ref, weight_ref, keep_ref, send_ref, *scratch):
    even_ref, odd_ref, total_ref, *fetched = scratch
    planes = own_ref.shape[0]
    group = weight_ref.shape[0] // 3
    kernel_ref, semaphores = fetched or (weight_ref, None)

    def fetch(step):
        where = pl.ds(step * group, group)
        return pltpu.make_async_copy(
            weight_ref.at[where], kernel_ref.at[where], semaphores.at[step]
        )

    if fetched:
        for step in range(3):
            fetch(step).start()
    place = lax.axis_index("depth")

    def plane_at(offset):
        if offset == 0:
            return jnp.where(place > 0, before_ref[planes - 1], 0.0)
        if offset == planes + 1:
            return jnp.where(place < lax.axis_size("depth") - 1, after_ref[0], 0.0)
        return own_ref[offset - 1]

    spread_field(plane_at, planes + 2, even_ref, odd_ref)
    total_ref[...] = jnp.zeros_like(total_ref)

    @pl.loop(0, 3)
    def _(step):
        if fetched:
            fetch(step).wait()
        kernels = kernel_ref.at[pl.ds(step * group, group)]
        total_ref[...] += back_step(2 - step, planes, kernels, even_ref, odd_ref)

    split_halves(total_ref[...].T, keep_ref, send_ref)


def full_spec(shape):
    return pl.BlockSpec(shape, lambda *_: (0,) * len(shape))


def spread_scratch(planes, height, breadth, lanes, parts):
    return [
        pltpu.VMEM((3, parts, planes, height // 2 + 1, 2 * breadth, lanes), jnp.bfloat16),
        pltpu.VMEM((3, parts, planes, height // 2, 2 * breadth, lanes), jnp.bfloat16),
    ]


def back_call(before, own, after, kernel, fetch):
    planes, height, breadth, lanes = own.shape
    taps, ins, outs = kernel.shape
    rows = planes * height * breadth
    shape = own.shape[:3] + (ins // 2,)
    return pl.pallas_call(
        back_kernel,
        in_specs=[pl.BlockSpec(memory_space=pltpu.VMEM)] * 3
        + [pl.BlockSpec(memory_space=pltpu.HBM if fetch else pltpu.VMEM)],
        out_shape=[jax.ShapeDtypeStruct(shape, jnp.float32)] * 2,
        scratch_shapes=spread_scratch(planes + 2, height, breadth, lanes, 2)
        + [pltpu.VMEM((ins, rows), jnp.float32)]
        + [pltpu.VMEM(kernel.shape, jnp.float32), pltpu.SemaphoreType.DMA((3,))] * fetch,
        compiler_params=pltpu.CompilerParams(vmem_limit_bytes=(14 if fetch else 10) * 2**20),
        cost_estimate=pl.CostEstimate(
            flops=6 * rows * taps * ins * outs, transcendentals=0, bytes_accessed=4 * kernel.size
        ),
    )(before, own, after, pltpu.with_memory_space_constraint(kernel, pltpu.HBM) if fetch else kernel)


def stage_kernel(inputs_ref, before_ref, grad_ref, both_ref, own_ref, semaphores):
    copies = [
        pltpu.make_async_copy(inputs_ref, both_ref.at[0], semaphores.at[0]),
        pltpu.make_async_copy(before_ref, both_ref.at[1], semaphores.at[1]),
        pltpu.make_async_copy(grad_ref, own_ref, semaphores.at[2]),
    ]
    for copy in copies:
        copy.start()
    for copy in copies:
        copy.wait()


def stage_call(inputs, before, grad):
    return pl.pallas_call(
        stage_kernel,
        in_specs=[pl.BlockSpec(memory_space=pltpu.HBM)] * 3,
        out_specs=[pl.BlockSpec(memory_space=pltpu.VMEM)] * 2,
        out_shape=[
            jax.ShapeDtypeStruct((2, *inputs.shape), jnp.float32),
            jax.ShapeDtypeStruct(grad.shape, jnp.float32),
        ],
        scratch_shapes=[pltpu.SemaphoreType.DMA((3,))],
        compiler_params=pltpu.CompilerParams(vmem_limit_bytes=2 * 2**20),
        name="stage",
    )(*(pltpu.with_memory_space_constraint(each, pltpu.HBM) for each in (inputs, before, grad)))


def join_kernel(*refs):
    *pieces, out_ref = refs
    count = len(pieces)
    planes = pieces[0].shape[0]
    place = lax.axis_index("depth")
    for step, piece in enumerate(pieces):
        source = lax.rem(place + count - step, count)
        out_ref[pl.ds(source * planes, planes)] = piece[...]


def join_depth(pieces):
    planes, *rest = pieces[0].shape
    return pl.pallas_call(
        join_kernel,
        out_shape=jax.ShapeDtypeStruct((planes * len(pieces), *rest), jnp.float32),
        compiler_params=pltpu.CompilerParams(vmem_limit_bytes=2 * 2**20),
        name="join_depth",
    )(*pieces)


def pair_kernel(count, *refs):
    fields, outs = refs[:count], refs[count:]
    depths = len(outs)
    place = lax.axis_index("depth")
    lanes = fields[0].shape[-1]
    half = lanes // 2
    for sample in range(count):
        shape = fields[sample].shape[1:]
        first = fields[sample][0].reshape(-1, lanes)
        activated, _ = gelu_pair(fields[sample][1].reshape(-1, lanes))
        lane = lax.broadcasted_iota(jnp.int32, first.shape, 1)
        low = jnp.where(lane < half, first, pltpu.roll(activated, half, axis=1)).reshape(shape)
        high = jnp.where(lane < half, pltpu.roll(first, half, axis=1), activated).reshape(shape)
        for step in range(depths):
            lower = lax.rem(place + step, 2) == 0
            outs[step][sample] = jnp.where(lower, low, high)


def pair_call(fields):
    depths, count = lax.axis_size("depth"), len(fields)
    shape = (count, *fields[0].shape[1:])
    return pl.pallas_call(
        functools.partial(pair_kernel, count),
        out_shape=[jax.ShapeDtypeStruct(shape, jnp.float32)] * depths,
        compiler_params=pltpu.CompilerParams(vmem_limit_bytes=6 * 2**20),
        name="pair",
    )(*fields)


def weight_kernel(count, second, factor, *refs):
    out_ref, even_ref, odd_ref, grad_ref = refs[-4:]
    fields, pairs = refs[:count], refs[count:-4]
    depths = len(pairs) // 2
    near, far = pairs[:depths], pairs[depths:]
    step = pl.program_id(0)
    planes, height, breadth, lanes = fields[0].shape
    share = planes // depths
    half = lanes // 2
    rows = planes * height * breadth

    @pl.when(step == 0)
    def _():
        place = lax.axis_index("depth")
        owner = place // 2 == lax.axis_index("filter")
        for sample in range(count):
            for ref in (even_ref, odd_ref):
                for tap in range(3):
                    for plane in (0, planes + 1):
                        ref[tap, sample, plane] = jnp.zeros(ref.shape[3:], ref.dtype)
            for hop, index in itertools.product(range(depths), range(share)):
                plane = lax.rem(place + depths - hop, depths) * share + index
                cells = jnp.where(owner, near[hop][sample, index], far[hop][sample, index])
                lane = lax.broadcasted_iota(jnp.int32, cells.shape, 2)
                swapped = pltpu.roll(cells, half, axis=2)
                lower = lane < half
                cells = jnp.where(lower, swapped, cells) if second else jnp.where(lower, cells, swapped)
                high = cells.astype(jnp.bfloat16).astype(jnp.float32)
                cells = jnp.where(lower, high, cells - high)
                for tap in range(3):
                    even, odd = row_pairs(column_shift(cells, tap))
                    even_ref[tap, sample, plane + 1] = even.astype(jnp.bfloat16)
                    odd_ref[tap, sample, plane + 1] = odd.astype(jnp.bfloat16)
            turned = fields[sample][...].reshape(rows, lanes).T
            for part, value in enumerate(two_parts(turned)):
                grad_ref[part * lanes : (part + 1) * lanes, sample * rows : (sample + 1) * rows] = value

    def cell(row_tap, column_tap):
        return jnp.concatenate(
            [
                slab(even_ref, odd_ref, (column_tap, sample), step, planes, row_tap)
                for sample in range(count)
            ],
            axis=0,
        )

    taps = [(row_tap, column_tap) for row_tap in range(3) for column_tap in range(3)]
    for start in range(0, 9, 2):
        group = taps[start : start + 2]
        right = [cell(*tap) for tap in group]
        right = jnp.concatenate(right, axis=1) if len(right) > 1 else right[0]
        product = jnp.dot(grad_ref[...], right, preferred_element_type=jnp.float32)
        product = product[:lanes] + product[lanes:]
        for index in range(len(group)):
            piece = product[:, index * lanes : (index + 1) * lanes]
            piece = piece + pltpu.roll(piece, half, axis=1)
            out_ref[start + index] = piece.T[:half] * factor


def weight_call(fields, near, far, second, factor):
    planes, height, breadth, lanes = fields[0].shape
    count = len(fields)
    rows = planes * height * breadth
    scratch = [
        pltpu.VMEM((3, count, planes + 2, height // 2 + 1, 2 * breadth, lanes), jnp.bfloat16),
        pltpu.VMEM((3, count, planes + 2, height // 2, 2 * breadth, lanes), jnp.bfloat16),
        pltpu.VMEM((2 * lanes, count * rows), jnp.bfloat16),
    ]
    return pl.pallas_call(
        functools.partial(weight_kernel, count, second, factor),
        grid=(3,),
        in_specs=[full_spec(each.shape) for each in (*fields, *near, *far)],
        out_specs=pl.BlockSpec((9, lanes // 2, lanes), lambda step: (step, 0, 0)),
        out_shape=jax.ShapeDtypeStruct((27, lanes // 2, lanes), jnp.float32),
        scratch_shapes=scratch,
        compiler_params=pltpu.CompilerParams(vmem_limit_bytes=20 * 2**20),
        cost_estimate=pl.CostEstimate(
            flops=4 * 2 * 27 * count * rows * lanes * lanes // 2,
            transcendentals=0,
            bytes_accessed=4 * 4 * count * rows * lanes,
        ),
        name="second_weight" if second else "first_weight",
    )(*fields, *near, *far)


def around_depth(field):
    count = lax.axis_size("depth")
    moved = {}
    for step in [1, count - 1] + list(range(2, count - 1)):
        links = [(i, (i + step) % count) for i in range(count)]
        moved[step] = lax.ppermute(field, "depth", links)
    return [field] + [moved[step] for step in range(1, count)]


def across_samples(field):
    count = lax.axis_size("sample")
    moved = [field]
    for step in range(1, count):
        moved.append(lax.ppermute(field, "sample", [(i, i ^ step) for i in range(count)]))
    return moved


def owners_around_depth(pairs):
    depths, samples, halves = axis_sizes()
    moved = [pairs[0]]
    for step in range(1, depths):
        links = []
        for depth, sample in itertools.product(range(depths), range(samples)):
            target = (depth + step) % depths
            half = target // 2
            place = lambda value: (value * samples + sample) * halves + half
            links.append((place(depth), place(target)))
        moved.append(lax.ppermute(pairs[step], ("depth", "sample", "filter"), links))
    return moved


def swap_filter(field):
    return lax.ppermute(field, "filter", [(0, 1), (1, 0)])


def gather_plan(inputs, pre_gelu, output_grad, first_weight, second_weight, factor):
    local_shape = output_grad.shape
    inputs, pre_gelu, output_grad = inputs[0], pre_gelu[0], output_grad[0]
    grads = around_depth(output_grad)
    both, grads[0] = stage_call(inputs, pre_gelu, output_grad)
    fields = across_samples(both)
    keep, send = back_call(grads[1], grads[0], grads[-1], second_weight, True)
    got = swap_filter(send)
    pre_grad = (keep + got) * gelu_pair(both[1])[1]
    grads = join_depth(grads)
    all_grads = across_samples(grads)
    pre_grads = around_depth(pre_grad)
    pairs = pair_call(fields)
    near = owners_around_depth(pairs)
    far = [swap_filter(piece) for piece in near]
    all_pre = across_samples(join_depth(pre_grads))
    keep, send = back_call(pre_grads[1], pre_grads[0], pre_grads[-1], first_weight, False)
    input_grad = (keep + swap_filter(send)).reshape(local_shape)
    second = weight_call(all_grads, near, far, True, factor)
    first = weight_call(all_pre, near, far, False, factor)
    return input_grad, first, second


def local(inputs, pre_gelu, output_grad, first_weight, second_weight):
    cells = (
        inputs.shape[0]
        * lax.axis_size("sample")
        * inputs.shape[1]
        * lax.axis_size("depth")
        * inputs.shape[2]
        * inputs.shape[3]
    )
    factor = 1.0 / math.sqrt(cells)
    if gather_plan_fits(output_grad, second_weight):
        return gather_plan(
            inputs, pre_gelu, output_grad, first_weight, second_weight, factor
        )
    activated, slope = gelu_pair(pre_gelu)
    stacked = jnp.stack([inputs, activated], axis=0)
    planes = padded_2(stacked, (("depth", 2),), 1)
    whole = lax.all_gather(planes, "filter", axis=5, tiled=True)
    padded = pad_sides(whole)
    local_width = output_grad.shape[4]
    act_columns = patches(padded[1], False)
    second_raw = jnp.einsum(
        "rti,rc->tic", act_columns, output_grad.reshape(-1, local_width), precision=highest
    )
    act_grad = spread_back(output_grad, second_weight)
    pre_grad = act_grad * slope
    input_grad = spread_back(pre_grad, first_weight)
    input_columns = patches(padded[0], False)
    first_raw = jnp.einsum(
        "rti,rc->tic", input_columns, pre_grad.reshape(-1, local_width), precision=highest
    )
    first_sum, second_sum = reduce_weight((first_raw, second_raw))
    return (input_grad, first_sum * factor, second_sum * factor)


def solution(mesh):
    return jax.shard_map(
        local,
        mesh=mesh,
        in_specs=(
            P("sample", "depth", None, None, "filter"),
            P("sample", "depth", None, None, "filter"),
            P("sample", "depth", None, None, "filter"),
            P(None, None, "filter"),
            P(None, None, "filter"),
        ),
        out_specs=(
            P("sample", "depth", None, None, "filter"),
            P(None, "depth", "filter"),
            P(None, "depth", "filter"),
        ),
        check_vma=False,
    )
```

```python
import functools
import itertools
import math

import jax
import jax.numpy as jnp
from jax import lax
from jax.experimental import pallas as pl
from jax.experimental.pallas import tpu as pltpu
from jax.sharding import PartitionSpec as P


highest = lax.Precision.HIGHEST


def padded_2(cells, sides, width):
    for axis, dim in sides:
        count = lax.axis_size(axis)
        ends = count - 1
        head = lax.slice_in_dim(cells, 0, width, axis=dim)
        tail = lax.slice_in_dim(cells, cells.shape[dim] - width, cells.shape[dim], axis=dim)
        cells = jnp.concatenate(
            [
                lax.ppermute(tail, axis, [(i, (i + 1) % count) for i in range(ends)]),
                cells,
                lax.ppermute(head, axis, [((i + 1) % count, i) for i in range(ends)]),
            ],
            axis=dim,
        )
    return cells


def gelu_pair(pre):
    normal_cdf = 0.5 * (1.0 + lax.erf(pre * 0.7071067811865476))
    density = jnp.exp(-0.5 * pre * pre) * 0.3989422804014327
    return (pre * normal_cdf, normal_cdf + pre * density)


def pad_sides(field):
    return jnp.pad(field, [(0, 0)] * (field.ndim - 3) + [(1, 1), (1, 1), (0, 0)])


def patches(padded, flipped):
    planes = padded.shape[-4] - 2
    height = padded.shape[-3] - 2
    breadth = padded.shape[-2] - 2
    pieces = []
    for depth_tap in range(3):
        for row_tap in range(3):
            for column_tap in range(3):
                start_plane = 2 - depth_tap if flipped else depth_tap
                start_row = 2 - row_tap if flipped else row_tap
                start_column = 2 - column_tap if flipped else column_tap
                pieces.append(
                    padded[
                        ...,
                        start_plane : start_plane + planes,
                        start_row : start_row + height,
                        start_column : start_column + breadth,
                        :,
                    ]
                )
    stacked = jnp.stack(pieces, axis=-2)
    return stacked.reshape(-1, 27, padded.shape[-1])


def spread_back(grad_local, kernel):
    planes = padded_2(grad_local, (("depth", 1),), 1)
    columns = patches(pad_sides(planes), True)
    partial_value = jnp.einsum("rtc,tic->ri", columns, kernel, precision=highest)
    partial_value = partial_value.reshape(grad_local.shape[:4] + (kernel.shape[1],))
    return lax.psum_scatter(partial_value, "filter", scatter_dimension=4, tiled=True)


def reduce_weight(raw_pair):
    summed = lax.psum(raw_pair, "sample")
    return lax.psum_scatter(summed, "depth", scatter_dimension=1, tiled=True)


def axis_sizes():
    return lax.axis_size("depth"), lax.axis_size("sample"), lax.axis_size("filter")


def gather_plan_fits(output_grad, second_weight):
    depths, samples, halves = axis_sizes()
    batch, planes, height, breadth, lanes = output_grad.shape
    rows = batch * samples * planes * depths * height * breadth
    return (
        batch == 1
        and halves == 2
        and lanes == 128
        and breadth == 8
        and height % 2 == 0
        and second_weight.shape[1] == halves * lanes
        and depths == 2 * halves
        and samples & (samples - 1) == 0
        and rows * lanes * 4 <= 2**21
    )


def column_shift(cells, tap):
    if tap == 1:
        return cells
    breadth = cells.shape[1]
    rolled = pltpu.roll(cells, 1 if tap == 0 else breadth - 1, axis=1)
    column = lax.broadcasted_iota(jnp.int32, cells.shape, 1)
    return jnp.where(column == (0 if tap == 0 else breadth - 1), 0.0, rolled)


def two_parts(cells):
    high = cells.astype(jnp.bfloat16)
    return high, (cells - high.astype(jnp.float32)).astype(jnp.bfloat16)


def row_pairs(cells):
    height, breadth, lanes = cells.shape
    edge = jnp.zeros((1, breadth, lanes), jnp.float32)
    even = jnp.concatenate([edge, cells, edge], axis=0)
    even = even.reshape(height // 2 + 1, 2 * breadth, lanes)
    return even, cells.reshape(height // 2, 2 * breadth, lanes)


def spread_field(get_plane, planes, even_ref, odd_ref):
    for plane in range(planes):
        source = get_plane(plane)
        for tap in range(3):
            even, odd = row_pairs(column_shift(source, tap))
            for part, value in enumerate(two_parts(even)):
                even_ref[tap, part, plane] = value
            for part, value in enumerate(two_parts(odd)):
                odd_ref[tap, part, plane] = value


def slab(even_ref, odd_ref, lead, first, planes, row_tap):
    pairs = odd_ref.shape[-3]
    where = pl.ds(first, planes)
    if row_tap == 1:
        value = odd_ref[(*lead, where)]
    else:
        start = row_tap // 2
        value = even_ref[(*lead, where, slice(start, start + pairs))]
    return value.reshape(-1, value.shape[-1])


def back_step(first, planes, weight_ref, even_ref, odd_ref):
    total = None
    for row_tap in range(3):
        cells = []
        kernels = []
        for column_tap in range(3):
            kernel_high, kernel_low = two_parts(weight_ref[3 * row_tap + column_tap])
            cell = [
                slab(even_ref, odd_ref, (2 - column_tap, part), first, planes, 2 - row_tap)
                for part in range(2)
            ]
            cells += [cell[0], cell[1], cell[0]]
            kernels += [kernel_high, kernel_high, kernel_low]
        product = lax.dot_general(
            jnp.concatenate(kernels, axis=1),
            jnp.concatenate(cells, axis=1),
            (((1,), (1,)), ((), ())),
            preferred_element_type=jnp.float32,
        )
        total = product if total is None else total + product
    return total


def split_halves(total, keep_ref, send_ref):
    width = keep_ref.shape[-1]
    mine = lax.axis_index("filter") == 0
    low, high = total[:, :width], total[:, width:]
    keep_ref[...] = jnp.where(mine, low, high).reshape(keep_ref.shape)
    send_ref[...] = jnp.where(mine, high, low).reshape(send_ref.shape)


def back_kernel(before_ref, own_ref, after_ref, weight_ref, keep_ref, send_ref, *scratch):
    even_ref, odd_ref, total_ref, *fetched = scratch
    planes = own_ref.shape[0]
    group = weight_ref.shape[0] // 3
    kernel_ref, semaphores = fetched or (weight_ref, None)

    def fetch(step):
        where = pl.ds(step * group, group)
        return pltpu.make_async_copy(
            weight_ref.at[where], kernel_ref.at[where], semaphores.at[step]
        )

    if fetched:
        for step in range(3):
            fetch(step).start()
    place = lax.axis_index("depth")

    def plane_at(offset):
        if offset == 0:
            return jnp.where(place > 0, before_ref[planes - 1], 0.0)
        if offset == planes + 1:
            return jnp.where(place < lax.axis_size("depth") - 1, after_ref[0], 0.0)
        return own_ref[offset - 1]

    spread_field(plane_at, planes + 2, even_ref, odd_ref)
    total_ref[...] = jnp.zeros_like(total_ref)

    @pl.loop(0, 3)
    def _(step):
        if fetched:
            fetch(step).wait()
        kernels = kernel_ref.at[pl.ds(step * group, group)]
        total_ref[...] += back_step(2 - step, planes, kernels, even_ref, odd_ref)

    split_halves(total_ref[...].T, keep_ref, send_ref)


def spread_scratch(planes, height, breadth, lanes, parts):
    return [
        pltpu.VMEM((3, parts, planes, height // 2 + 1, 2 * breadth, lanes), jnp.bfloat16),
        pltpu.VMEM((3, parts, planes, height // 2, 2 * breadth, lanes), jnp.bfloat16),
    ]


def back_call(before, own, after, kernel, fetch):
    planes, height, breadth, lanes = own.shape
    taps, ins, outs = kernel.shape
    rows = planes * height * breadth
    shape = own.shape[:3] + (ins // 2,)
    return pl.pallas_call(
        back_kernel,
        in_specs=[pl.BlockSpec(memory_space=pltpu.VMEM)] * 3
        + [pl.BlockSpec(memory_space=pltpu.HBM if fetch else pltpu.VMEM)],
        out_shape=[jax.ShapeDtypeStruct(shape, jnp.float32)] * 2,
        scratch_shapes=spread_scratch(planes + 2, height, breadth, lanes, 2)
        + [pltpu.VMEM((ins, rows), jnp.float32)]
        + [pltpu.VMEM(kernel.shape, jnp.float32), pltpu.SemaphoreType.DMA((3,))] * fetch,
        compiler_params=pltpu.CompilerParams(vmem_limit_bytes=(14 if fetch else 10) * 2**20),
        cost_estimate=pl.CostEstimate(
            flops=6 * rows * taps * ins * outs, transcendentals=0, bytes_accessed=4 * kernel.size
        ),
    )(before, own, after, pltpu.with_memory_space_constraint(kernel, pltpu.HBM) if fetch else kernel)


def stage_kernel(inputs_ref, before_ref, grad_ref, both_ref, own_ref, semaphores):
    copies = [
        pltpu.make_async_copy(inputs_ref, both_ref.at[0], semaphores.at[0]),
        pltpu.make_async_copy(before_ref, both_ref.at[1], semaphores.at[1]),
        pltpu.make_async_copy(grad_ref, own_ref, semaphores.at[2]),
    ]
    for copy in copies:
        copy.start()
    for copy in copies:
        copy.wait()


def stage_call(inputs, before, grad):
    return pl.pallas_call(
        stage_kernel,
        in_specs=[pl.BlockSpec(memory_space=pltpu.HBM)] * 3,
        out_specs=[pl.BlockSpec(memory_space=pltpu.VMEM)] * 2,
        out_shape=[
            jax.ShapeDtypeStruct((2, *inputs.shape), jnp.float32),
            jax.ShapeDtypeStruct(grad.shape, jnp.float32),
        ],
        scratch_shapes=[pltpu.SemaphoreType.DMA((3,))],
        compiler_params=pltpu.CompilerParams(vmem_limit_bytes=2 * 2**20),
        name="stage",
    )(*(pltpu.with_memory_space_constraint(each, pltpu.HBM) for each in (inputs, before, grad)))


def join_kernel(*refs):
    *pieces, out_ref = refs
    count = len(pieces)
    planes = pieces[0].shape[0]
    place = lax.axis_index("depth")
    for step, piece in enumerate(pieces):
        source = lax.rem(place + count - step, count)
        out_ref[pl.ds(source * planes, planes)] = piece[...]


def join_depth(pieces):
    planes, *rest = pieces[0].shape
    return pl.pallas_call(
        join_kernel,
        out_shape=jax.ShapeDtypeStruct((planes * len(pieces), *rest), jnp.float32),
        compiler_params=pltpu.CompilerParams(vmem_limit_bytes=2 * 2**20),
        name="join_depth",
    )(*pieces)


def pair_kernel(count, *refs):
    fields, outs = refs[:count], refs[count:]
    place = lax.axis_index("depth")
    inside = place // 2 == lax.axis_index("filter")
    targets = (place, place ^ jnp.where(inside, 1, 2), place ^ 3)
    lanes = fields[0].shape[-1]
    half = lanes // 2
    for sample in range(count):
        shape = fields[sample].shape[1:]
        first = fields[sample][0].reshape(-1, lanes)
        activated, _ = gelu_pair(fields[sample][1].reshape(-1, lanes))
        lane = lax.broadcasted_iota(jnp.int32, first.shape, 1)
        low = jnp.where(lane < half, first, pltpu.roll(activated, half, axis=1)).reshape(shape)
        high = jnp.where(lane < half, pltpu.roll(first, half, axis=1), activated).reshape(shape)
        for out, target in zip(outs, targets):
            out[sample] = jnp.where(target % 2 == 0, low, high)


def pair_call(fields):
    shape = (len(fields), *fields[0].shape[1:])
    return pl.pallas_call(
        functools.partial(pair_kernel, len(fields)),
        out_shape=[jax.ShapeDtypeStruct(shape, jnp.float32)] * 3,
        compiler_params=pltpu.CompilerParams(vmem_limit_bytes=6 * 2**20),
        name="pair",
    )(*fields)


def weight_kernel(count, second, factor, *refs):
    out_ref, even_ref, odd_ref, grad_ref, done_ref, semaphores = refs[-6:]
    fields, pairs = refs[:count], refs[count:-6]
    depths = len(pairs) // 2
    near, far = pairs[:depths], pairs[depths:]
    planes, height, breadth, lanes = fields[0].shape
    share = planes // depths
    half = lanes // 2
    rows = planes * height * breadth

    place = lax.axis_index("depth")
    owner = place // 2 == lax.axis_index("filter")
    for sample in range(count):
        for ref in (even_ref, odd_ref):
            for tap in range(3):
                for plane in (0, planes + 1):
                    ref[tap, sample, plane] = jnp.zeros(ref.shape[3:], ref.dtype)
        for hop, index in itertools.product(range(depths), range(share)):
            plane = (place ^ hop) * share + index
            cells = jnp.where(owner, near[hop][sample, index], far[hop][sample, index])
            lane = lax.broadcasted_iota(jnp.int32, cells.shape, 2)
            swapped = pltpu.roll(cells, half, axis=2)
            lower = lane < half
            cells = jnp.where(lower, swapped, cells) if second else jnp.where(lower, cells, swapped)
            high = cells.astype(jnp.bfloat16).astype(jnp.float32)
            cells = jnp.where(lower, high, cells - high)
            for tap in range(3):
                even, odd = row_pairs(column_shift(cells, tap))
                even_ref[tap, sample, plane + 1] = even.astype(jnp.bfloat16)
                odd_ref[tap, sample, plane + 1] = odd.astype(jnp.bfloat16)
        turned = fields[sample][...].reshape(rows, lanes).T
        for part, value in enumerate(two_parts(turned)):
            grad_ref[part * lanes : (part + 1) * lanes, sample * rows : (sample + 1) * rows] = value

    def cell(depth_tap, row_tap, column_tap):
        return jnp.concatenate(
            [
                slab(even_ref, odd_ref, (column_tap, sample), depth_tap, planes, row_tap)
                for sample in range(count)
            ],
            axis=0,
        )

    def deliver(third):
        where = pl.ds(9 * third, 9)
        return pltpu.make_async_copy(done_ref.at[where], out_ref.at[where], semaphores.at[third])

    taps = list(itertools.product(range(3), repeat=3))
    for start in range(0, 27, 4):
        group = taps[start : start + 4]
        right = jnp.concatenate([cell(*tap) for tap in group], axis=1)
        product = jnp.dot(grad_ref[...], right, preferred_element_type=jnp.float32)
        product = product[:lanes] + product[lanes:]
        for index in range(len(group)):
            piece = product[:, index * lanes : (index + 1) * lanes]
            piece = piece + pltpu.roll(piece, half, axis=1)
            done_ref[start + index] = piece.T[:half] * factor
            if (start + index) % 9 == 8:
                deliver((start + index) // 9).start()
    for third in range(3):
        deliver(third).wait()


def weight_call(fields, near, far, second, factor):
    planes, height, breadth, lanes = fields[0].shape
    count = len(fields)
    rows = planes * height * breadth
    scratch = [
        pltpu.VMEM((3, count, planes + 2, height // 2 + 1, 2 * breadth, lanes), jnp.bfloat16),
        pltpu.VMEM((3, count, planes + 2, height // 2, 2 * breadth, lanes), jnp.bfloat16),
        pltpu.VMEM((2 * lanes, count * rows), jnp.bfloat16),
        pltpu.VMEM((27, lanes // 2, lanes), jnp.float32),
        pltpu.SemaphoreType.DMA((3,)),
    ]
    return pl.pallas_call(
        functools.partial(weight_kernel, count, second, factor),
        in_specs=[pl.BlockSpec(memory_space=pltpu.VMEM)] * (len(fields) + 2 * len(near)),
        out_specs=pl.BlockSpec(memory_space=pltpu.HBM),
        out_shape=jax.ShapeDtypeStruct((27, lanes // 2, lanes), jnp.float32),
        scratch_shapes=scratch,
        compiler_params=pltpu.CompilerParams(vmem_limit_bytes=20 * 2**20),
        cost_estimate=pl.CostEstimate(
            flops=4 * 2 * 27 * count * rows * lanes * lanes // 2,
            transcendentals=0,
            bytes_accessed=4 * 4 * count * rows * lanes,
        ),
        name="second_weight" if second else "first_weight",
    )(*fields, *near, *far)


def around_depth(field):
    count = lax.axis_size("depth")
    moved = {}
    for step in [1, count - 1] + list(range(2, count - 1)):
        links = [(i, (i + step) % count) for i in range(count)]
        moved[step] = lax.ppermute(field, "depth", links)
    return [field] + [moved[step] for step in range(1, count)]


def across_samples(field):
    count = lax.axis_size("sample")
    moved = [field]
    for step in range(1, count):
        moved.append(lax.ppermute(field, "sample", [(i, i ^ step) for i in range(count)]))
    return moved


def pairs_around_depth(pairs):
    depths, samples, halves = axis_sizes()
    place = lambda depth, sample, half: (depth * samples + sample) * halves + half
    links = [], []
    for depth, sample, half in itertools.product(range(depths), range(samples), range(halves)):
        source = place(depth, sample, half)
        if depth // 2 == half:
            links[0].append((source, place(depth ^ 1, sample, half)))
        else:
            links[0].append((source, place(depth ^ 2, sample, 1 - half)))
            links[1].append((source, place(depth ^ 3, sample, half)))
    own, *moved = pairs
    for index in range(2):
        axes = ("depth", "sample", "filter")
        moved[index] = lax.ppermute(moved[index], axes, links[index])
    swapped = [swap_filter(piece) for piece in (own, *moved)]
    near = [own, moved[0], swapped[1], moved[1]]
    far = [swapped[0], swapped[1], moved[0], swapped[2]]
    return near, far


def swap_filter(field):
    return lax.ppermute(field, "filter", [(0, 1), (1, 0)])


def gather_plan(inputs, pre_gelu, output_grad, first_weight, second_weight, factor):
    local_shape = output_grad.shape
    inputs, pre_gelu, output_grad = inputs[0], pre_gelu[0], output_grad[0]
    grads = around_depth(output_grad)
    both, grads[0] = stage_call(inputs, pre_gelu, output_grad)
    fields = across_samples(both)
    keep, send = back_call(grads[1], grads[0], grads[-1], second_weight, True)
    got = swap_filter(send)
    pre_grad = (keep + got) * gelu_pair(both[1])[1]
    grads = join_depth(grads)
    all_grads = across_samples(grads)
    pre_grads = around_depth(pre_grad)
    pairs = pair_call(fields)
    near, far = pairs_around_depth(pairs)
    all_pre = across_samples(join_depth(pre_grads))
    keep, send = back_call(pre_grads[1], pre_grads[0], pre_grads[-1], first_weight, False)
    input_grad = (keep + swap_filter(send)).reshape(local_shape)
    second = weight_call(all_grads, near, far, True, factor)
    first = weight_call(all_pre, near, far, False, factor)
    return input_grad, first, second


def local(inputs, pre_gelu, output_grad, first_weight, second_weight):
    cells = (
        inputs.shape[0]
        * lax.axis_size("sample")
        * inputs.shape[1]
        * lax.axis_size("depth")
        * inputs.shape[2]
        * inputs.shape[3]
    )
    factor = 1.0 / math.sqrt(cells)
    if gather_plan_fits(output_grad, second_weight):
        return gather_plan(
            inputs, pre_gelu, output_grad, first_weight, second_weight, factor
        )
    activated, slope = gelu_pair(pre_gelu)
    stacked = jnp.stack([inputs, activated], axis=0)
    planes = padded_2(stacked, (("depth", 2),), 1)
    whole = lax.all_gather(planes, "filter", axis=5, tiled=True)
    padded = pad_sides(whole)
    local_width = output_grad.shape[4]
    act_columns = patches(padded[1], False)
    second_raw = jnp.einsum(
        "rti,rc->tic", act_columns, output_grad.reshape(-1, local_width), precision=highest
    )
    act_grad = spread_back(output_grad, second_weight)
    pre_grad = act_grad * slope
    input_grad = spread_back(pre_grad, first_weight)
    input_columns = patches(padded[0], False)
    first_raw = jnp.einsum(
        "rti,rc->tic", input_columns, pre_grad.reshape(-1, local_width), precision=highest
    )
    first_sum, second_sum = reduce_weight((first_raw, second_raw))
    return (input_grad, first_sum * factor, second_sum * factor)


def solution(mesh):
    return jax.shard_map(
        local,
        mesh=mesh,
        in_specs=(
            P("sample", "depth", None, None, "filter"),
            P("sample", "depth", None, None, "filter"),
            P("sample", "depth", None, None, "filter"),
            P(None, None, "filter"),
            P(None, None, "filter"),
        ),
        out_specs=(
            P("sample", "depth", None, None, "filter"),
            P(None, "depth", "filter"),
            P(None, "depth", "filter"),
        ),
        check_vma=False,
    )
```
